32 devices in a mesh: dp: 4 (over z), ring: 2 (over y), uly: 4 (over x, core).
Axes of the slice: x: 2, y: 2, z: 4, core: 2. Of those that a mesh axis runs over, the one named last changes fastest.
Arguments:
- y_mod: bfloat16 [4, 8192, 1536], P('dp', ('ring', 'uly'))
- pre_q: bfloat16 [4, 8192, 1536], P('dp', ('ring', 'uly'))
- pre_k: bfloat16 [4, 8192, 1536], P('dp', ('ring', 'uly'))
- inv_q: float32 [4, 8192], P('dp', ('ring', 'uly'))
- inv_k: float32 [4, 8192], P('dp', ('ring', 'uly'))
- log_sum: float32 [4, 12, 8192], P('dp', None, ('ring', 'uly'))
- attn_out: bfloat16 [4, 8192, 1536], P('dp', ('ring', 'uly'))
- gate_msa: float32 [4, 1536], P('dp')
- d_resid: bfloat16 [4, 8192, 1536], P('dp', ('ring', 'uly'))
- angles: float32 [8192, 64], P(('ring', 'uly'))
- w_q: bfloat16 [1536, 1536], replicated
- w_k: bfloat16 [1536, 1536], replicated
- w_v: bfloat16 [1536, 1536], replicated
- b_v: float32 [1536], replicated
- w_o: bfloat16 [1536, 1536], replicated
- g_q: float32 [1536], replicated
- g_k: float32 [1536], replicated
Outputs:
- output 1: bfloat16 [4, 8192, 1536], P('dp', ('ring', 'uly'))
- output 2: float32 [1536, 1536], replicated
- output 3: float32 [1536, 1536], replicated
- output 4: float32 [1536, 1536], replicated
- output 5: float32 [1536, 1536], replicated
- output 6: float32 [1536], replicated
- output 7: float32 [1536], replicated
- output 8: float32 [1536], replicated
- output 9: float32 [1536], replicated
- output 10: float32 [1536], replicated
- output 11: float32 [1536], replicated
All inputs are finite; a program needn't handle non-finite values.
Results may differ from the reference program's by a relative error of at most 0.00911088.
Values are sent between devices in bfloat16 or wider.
A program may use at most 1 GiB of HBM per device.

```python
import jax
import jax.numpy as jnp
from jax import lax

BATCH = 4
SEQ_LEN = 8192
MODEL_WIDTH = 1536
HEADS = 12
HEAD_DIM = 128
QUERY_BLOCK = 256
NORM_EPS = 1e-6
ROPE_BASE = 10000.0


def rope_turn(feats, cos_tab, sin_tab):
    pairs = feats.reshape(feats.shape[:-1] + (HEAD_DIM // 2, 2))
    even_part = pairs[..., 0]
    odd_part = pairs[..., 1]
    cos_b = cos_tab[:, None, :]
    sin_b = sin_tab[:, None, :]
    turned = jnp.stack([even_part * cos_b - odd_part * sin_b, even_part * sin_b + odd_part * cos_b], axis=-1)
    return turned.reshape(feats.shape)


def norm_rope(proj, inv_rms, gain, angles):
    normed = proj.astype(jnp.float32) * inv_rms[..., None] * gain
    heads_view = normed.reshape(normed.shape[:-1] + (HEADS, HEAD_DIM))
    turned = rope_turn(heads_view, jnp.cos(angles), jnp.sin(angles))
    return turned.reshape(normed.shape).astype(jnp.bfloat16)


def value_proj(flat_y, w_v, b_v):
    out_rows = jnp.dot(flat_y, w_v, preferred_element_type=jnp.float32) + b_v
    return out_rows.astype(jnp.bfloat16).reshape(BATCH, SEQ_LEN, MODEL_WIDTH)


def to_heads(arr):
    return jnp.transpose(arr.reshape(BATCH, SEQ_LEN, HEADS, HEAD_DIM), (0, 2, 1, 3)).reshape(BATCH * HEADS, SEQ_LEN, HEAD_DIM)


def from_heads(arr):
    return jnp.transpose(arr.reshape(BATCH, HEADS, SEQ_LEN, HEAD_DIM), (0, 2, 1, 3)).reshape(BATCH, SEQ_LEN, MODEL_WIDTH)


def head_forward(head_args):
    q_head, k_head, v_head = head_args
    score_scale = HEAD_DIM ** -0.5
    n_blocks = SEQ_LEN // QUERY_BLOCK

    def blk_fwd(q_blk):
        scores = jnp.dot(q_blk, k_head.T, preferred_element_type=jnp.float32) * score_scale
        row_max = jnp.max(scores, axis=-1, keepdims=True)
        exp_scores = jnp.exp(scores - row_max)
        row_total = jnp.sum(exp_scores, axis=-1, keepdims=True)
        blk_out = jnp.dot(exp_scores / row_total, v_head.astype(jnp.float32))
        return blk_out, (row_max + jnp.log(row_total))[:, 0]

    out_blocks, lse_blocks = lax.map(blk_fwd, q_head.reshape(n_blocks, QUERY_BLOCK, HEAD_DIM))
    return out_blocks.reshape(SEQ_LEN, HEAD_DIM), lse_blocks.reshape(SEQ_LEN)


def forward_saved(y_mod, w_q, b_q, w_k, b_k, w_v, b_v, g_q, g_k, angles):
    flat_y = y_mod.reshape(BATCH * SEQ_LEN, MODEL_WIDTH)
    pre_q = (jnp.dot(flat_y, w_q, preferred_element_type=jnp.float32) + b_q).astype(jnp.bfloat16).reshape(BATCH, SEQ_LEN, MODEL_WIDTH)
    pre_k = (jnp.dot(flat_y, w_k, preferred_element_type=jnp.float32) + b_k).astype(jnp.bfloat16).reshape(BATCH, SEQ_LEN, MODEL_WIDTH)
    inv_q = lax.rsqrt(jnp.mean(jnp.square(pre_q.astype(jnp.float32)), axis=-1) + NORM_EPS)
    inv_k = lax.rsqrt(jnp.mean(jnp.square(pre_k.astype(jnp.float32)), axis=-1) + NORM_EPS)
    q_rot = norm_rope(pre_q, inv_q, g_q, angles)
    k_rot = norm_rope(pre_k, inv_k, g_k, angles)
    v_proj = value_proj(flat_y, w_v, b_v)
    attn_heads, lse_heads = lax.map(head_forward, (to_heads(q_rot), to_heads(k_rot), to_heads(v_proj)))
    attn_out = from_heads(attn_heads).astype(jnp.bfloat16)
    log_sum = lse_heads.reshape(BATCH, HEADS, SEQ_LEN)
    return pre_q, pre_k, inv_q, inv_k, attn_out, log_sum


def setup_inputs(seed: int = 0) -> dict:
    sub_keys = jax.random.split(jax.random.key(seed), 14)
    in_scale = MODEL_WIDTH ** -0.5
    shape3 = (BATCH, SEQ_LEN, MODEL_WIDTH)
    wshape = (MODEL_WIDTH, MODEL_WIDTH)
    y_mod = jax.random.normal(sub_keys[0], shape3, jnp.float32).astype(jnp.bfloat16)
    w_q = (jax.random.normal(sub_keys[1], wshape, jnp.float32) * in_scale).astype(jnp.bfloat16)
    w_k = (jax.random.normal(sub_keys[2], wshape, jnp.float32) * in_scale).astype(jnp.bfloat16)
    w_v = (jax.random.normal(sub_keys[3], wshape, jnp.float32) * in_scale).astype(jnp.bfloat16)
    w_o = (jax.random.normal(sub_keys[4], wshape, jnp.float32) * in_scale).astype(jnp.bfloat16)
    b_q = 0.5 * jax.random.normal(sub_keys[5], (MODEL_WIDTH,), jnp.float32)
    b_k = 0.5 * jax.random.normal(sub_keys[6], (MODEL_WIDTH,), jnp.float32)
    b_v = 0.5 * jax.random.normal(sub_keys[7], (MODEL_WIDTH,), jnp.float32)
    g_q = 1.6 + 0.2 * jax.random.normal(sub_keys[8], (MODEL_WIDTH,), jnp.float32)
    g_k = 1.6 + 0.2 * jax.random.normal(sub_keys[9], (MODEL_WIDTH,), jnp.float32)
    gate_msa = 1.0 + 0.5 * jax.random.normal(sub_keys[10], (BATCH, MODEL_WIDTH), jnp.float32)
    d_resid = jax.random.normal(sub_keys[11], shape3, jnp.float32).astype(jnp.bfloat16)
    positions = jax.random.randint(sub_keys[12], (SEQ_LEN,), 0, 4096)
    rope_freqs = ROPE_BASE ** (-2.0 * jnp.arange(HEAD_DIM // 2, dtype=jnp.float32) / HEAD_DIM)
    angles = positions.astype(jnp.float32)[:, None] * rope_freqs[None, :]
    pre_q, pre_k, inv_q, inv_k, attn_out, log_sum = forward_saved(y_mod, w_q, b_q, w_k, b_k, w_v, b_v, g_q, g_k, angles)
    return {'y_mod': y_mod, 'pre_q': pre_q, 'pre_k': pre_k, 'inv_q': inv_q, 'inv_k': inv_k, 'log_sum': log_sum, 'attn_out': attn_out, 'gate_msa': gate_msa, 'd_resid': d_resid, 'angles': angles, 'w_q': w_q, 'w_k': w_k, 'w_v': w_v, 'b_v': b_v, 'w_o': w_o, 'g_q': g_q, 'g_k': g_k}


def head_backward(head_args):
    q_head, k_head, v_head, da_head, lse_head, dot_head = head_args
    score_scale = HEAD_DIM ** -0.5
    n_blocks = SEQ_LEN // QUERY_BLOCK

    def blk_back(acc_state, blk_args):
        dk_acc, dv_acc = acc_state
        q_blk, da_blk, lse_blk, dot_blk = blk_args
        scores = jnp.dot(q_blk, k_head.T, preferred_element_type=jnp.float32) * score_scale
        p_mat = jnp.exp(scores - lse_blk[:, None])
        p_low = p_mat.astype(jnp.bfloat16)
        dv_acc = dv_acc + jnp.dot(p_low.T, da_blk, preferred_element_type=jnp.float32)
        dp_mat = jnp.dot(da_blk, v_head.T, preferred_element_type=jnp.float32)
        ds_low = (p_mat * (dp_mat - dot_blk[:, None])).astype(jnp.bfloat16)
        dq_blk = jnp.dot(ds_low, k_head, preferred_element_type=jnp.float32) * score_scale
        dk_acc = dk_acc + jnp.dot(ds_low.T, q_blk, preferred_element_type=jnp.float32) * score_scale
        return (dk_acc, dv_acc), dq_blk

    zero_acc = jnp.zeros((SEQ_LEN, HEAD_DIM), jnp.float32)
    blk_inputs = (q_head.reshape(n_blocks, QUERY_BLOCK, HEAD_DIM), da_head.reshape(n_blocks, QUERY_BLOCK, HEAD_DIM), lse_head.reshape(n_blocks, QUERY_BLOCK), dot_head.reshape(n_blocks, QUERY_BLOCK))
    (dk_head, dv_head), dq_blocks = lax.scan(blk_back, (zero_acc, zero_acc), blk_inputs)
    return dq_blocks.reshape(SEQ_LEN, HEAD_DIM), dk_head, dv_head


def norm_back(d_norm, proj, inv_rms, gain):
    proj_f = proj.astype(jnp.float32)
    rms_b = inv_rms[..., None]
    d_gain = jnp.sum(d_norm * proj_f * rms_b, axis=(0, 1))
    mixed = jnp.mean(proj_f * gain * d_norm, axis=-1, keepdims=True)
    d_proj = rms_b * gain * d_norm - proj_f * rms_b ** 3 * mixed
    return d_proj.astype(jnp.bfloat16), d_gain


def reference(y_mod, pre_q, pre_k, inv_q, inv_k, log_sum, attn_out, gate_msa, d_resid, angles, w_q, w_k, w_v, b_v, w_o, g_q, g_k):
    n_rows = BATCH * SEQ_LEN
    flat_y = y_mod.reshape(n_rows, MODEL_WIDTH)
    d_out = (d_resid.astype(jnp.float32) * gate_msa[:, None, :]).astype(jnp.bfloat16).reshape(n_rows, MODEL_WIDTH)
    flat_attn = attn_out.reshape(n_rows, MODEL_WIDTH)
    dw_o = jnp.dot(flat_attn.T, d_out, preferred_element_type=jnp.float32)
    db_o = jnp.sum(d_out.astype(jnp.float32), axis=0)
    d_attn = jnp.dot(d_out, w_o.T, preferred_element_type=jnp.float32).astype(jnp.bfloat16).reshape(BATCH, SEQ_LEN, MODEL_WIDTH)
    q_rot = norm_rope(pre_q, inv_q, g_q, angles)
    k_rot = norm_rope(pre_k, inv_k, g_k, angles)
    v_proj = value_proj(flat_y, w_v, b_v)
    row_dot = jnp.sum((d_attn.astype(jnp.float32) * attn_out.astype(jnp.float32)).reshape(BATCH, SEQ_LEN, HEADS, HEAD_DIM), axis=-1)
    dot_heads = jnp.transpose(row_dot, (0, 2, 1)).reshape(BATCH * HEADS, SEQ_LEN)
    lse_heads = log_sum.reshape(BATCH * HEADS, SEQ_LEN)
    dq_h, dk_h, dv_h = lax.map(head_backward, (to_heads(q_rot), to_heads(k_rot), to_heads(v_proj), to_heads(d_attn), lse_heads, dot_heads))
    dq_low = from_heads(dq_h).astype(jnp.bfloat16)
    dk_low = from_heads(dk_h).astype(jnp.bfloat16)
    dv_low = from_heads(dv_h).astype(jnp.bfloat16)
    cos_tab = jnp.cos(angles)
    sin_tab = jnp.sin(angles)
    head_shape = (BATCH, SEQ_LEN, HEADS, HEAD_DIM)
    full_shape = (BATCH, SEQ_LEN, MODEL_WIDTH)
    dq_norm = rope_turn(dq_low.astype(jnp.float32).reshape(head_shape), cos_tab, -sin_tab).reshape(full_shape)
    dk_norm = rope_turn(dk_low.astype(jnp.float32).reshape(head_shape), cos_tab, -sin_tab).reshape(full_shape)
    d_preq, dg_q = norm_back(dq_norm, pre_q, inv_q, g_q)
    d_prek, dg_k = norm_back(dk_norm, pre_k, inv_k, g_k)
    flat_dq = d_preq.reshape(n_rows, MODEL_WIDTH)
    flat_dk = d_prek.reshape(n_rows, MODEL_WIDTH)
    flat_dv = dv_low.reshape(n_rows, MODEL_WIDTH)
    dw_q = jnp.dot(flat_y.T, flat_dq, preferred_element_type=jnp.float32)
    dw_k = jnp.dot(flat_y.T, flat_dk, preferred_element_type=jnp.float32)
    dw_v = jnp.dot(flat_y.T, flat_dv, preferred_element_type=jnp.float32)
    db_q = jnp.sum(flat_dq.astype(jnp.float32), axis=0)
    db_k = jnp.sum(flat_dk.astype(jnp.float32), axis=0)
    db_v = jnp.sum(flat_dv.astype(jnp.float32), axis=0)
    grad_rows = jnp.dot(flat_dq, w_q.T, preferred_element_type=jnp.float32) + jnp.dot(flat_dk, w_k.T, preferred_element_type=jnp.float32) + jnp.dot(flat_dv, w_v.T, preferred_element_type=jnp.float32)
    grad_y = grad_rows.astype(jnp.bfloat16).reshape(full_shape)
    return (grad_y, dw_q, dw_k, dw_v, dw_o, db_q, db_k, db_v, db_o, dg_q, dg_k)
```

```python
import functools

import jax
import jax.numpy as jnp
from jax import lax
from jax.experimental import pallas as pl
from jax.experimental.pallas import tpu as pltpu
from jax.sharding import PartitionSpec as P


F32 = jnp.float32
BF16 = jnp.bfloat16
LOG2E = 1.4426950408889634
GROUP = ('ring', 'uly')
VMEM_LIMIT = 66 * 1000 * 1000
BY_TRANSPOSE = (((1,), (1,)), ((), ()))
NQ_BLK = 1024
NK_BLK = 512
UNROLL = 2


def split3(col):
    hi = col.astype(BF16)
    rest = col - hi.astype(F32)
    mid = rest.astype(BF16)
    low = (rest - mid.astype(F32)).astype(BF16)
    return hi, mid, low


def ext_cols(col, lane):
    hi, mid, low = (x.astype(F32) for x in split3(col))
    return jnp.where(lane == 0, hi, jnp.where(lane == 1, mid, jnp.where(lane == 2, low, 0.0))).astype(BF16)


def rope_tables(cs, half):
    width = 2 * half
    row = lax.broadcasted_iota(jnp.int32, (width, width), 0)
    col = lax.broadcasted_iota(jnp.int32, (width, width), 1)
    pick_c = jnp.where(row == col // 2, 1.0, 0.0).astype(BF16)
    sign = jnp.where(col % 2 == 0, -1.0, 1.0)
    pick_s = jnp.where(row == half + col // 2, sign, 0.0).astype(BF16)
    pieces = split3(cs)
    cos_t = sum(jnp.dot(x, pick_c, preferred_element_type=F32) for x in pieces)
    sin_t = sum(jnp.dot(x, pick_s, preferred_element_type=F32) for x in pieces)
    return cos_t, sin_t


def swap_pairs(x, lane):
    width = x.shape[-1]
    return jnp.where(lane % 2 == 0, pltpu.roll(x, width - 1, 1), pltpu.roll(x, 1, 1))


def attn_kernel(scale, whole_q, n_qp, *refs):
    in_refs, refs = refs[:n_qp], refs[n_qp:]
    (stat_ref, gain_ref, cs_ref), refs = refs[:3], refs[3:]
    dq_refs, refs = refs[:n_qp], refs[n_qp:]
    dk_ref, dv_ref, qx, dax, kx, vx, qt, dat, kr, dkt, dvt, in_buf, in_sem, cs_buf, cs_sem = refs
    n_part, tok, dim = dq_refs[0].shape
    n_kb = dk_ref.shape[0]
    half = dim // 2
    lane = lax.broadcasted_iota(jnp.int32, (tok, dim), 1)
    sub = lax.broadcasted_iota(jnp.int32, (dim, tok), 0)
    ones = jnp.where(sub < 3, 1.0, 0.0).astype(BF16)
    lse_t = jnp.transpose(stat_ref[0]) * (-1.0 / scale)
    del_t = jnp.transpose(stat_ref[1]) * -1.0
    ivq_t = jnp.transpose(stat_ref[2])
    ivk_t = jnp.transpose(stat_ref[3])
    gain_q = gain_ref[0:1, :]
    gain_k = gain_ref[1:2, :]

    def in_copy(blk):
        src = in_refs[blk // n_part].at[blk % n_part]
        return pltpu.make_async_copy(src, in_buf.at[blk % 2, pl.ds(0, src.shape[0])], in_sem.at[blk % 2])

    def cs_copy(blk):
        return pltpu.make_async_copy(cs_ref.at[blk], cs_buf.at[blk % 2], cs_sem.at[blk % 2])

    def tables(blk, last):
        cs_copy(blk).wait()
        found = rope_tables(cs_buf[blk % 2], half)
        if blk + 2 <= last:
            cs_copy(blk + 2).start()
        return found

    def turned(pre, inv_col, gain, cos_t, sin_t):
        normed = pre.astype(F32) * inv_col * gain
        return (normed * cos_t + swap_pairs(normed, lane) * sin_t).astype(BF16)

    n_qb = n_qp * n_part
    in_copy(0).start()
    cs_copy(0).start()
    cs_copy(1).start()
    for blk in range(n_qp * n_part):
        rows = slice(blk * tok, (blk + 1) * tok)
        cos_t, sin_t = tables(blk, n_qb - 1)
        in_copy(blk).wait()
        if blk + 1 < n_qb:
            in_copy(blk + 1).start()
        slot = blk % 2
        q_blk = turned(in_buf[slot, 0], ivq_t[:, blk:blk + 1], gain_q, cos_t, sin_t)
        da_blk = in_buf[slot, 1]
        qx[rows, :dim] = q_blk
        qx[rows, dim:] = ext_cols(jnp.broadcast_to(lse_t[:, blk:blk + 1], (tok, dim)), lane)
        dax[rows, :dim] = da_blk
        dax[rows, dim:] = ext_cols(jnp.broadcast_to(del_t[:, blk:blk + 1], (tok, dim)), lane)
        qt[:, rows] = jnp.transpose(q_blk)
        dat[:, rows] = jnp.transpose(da_blk)
        if blk < n_kb:
            k_blk = turned(in_buf[slot, 2], ivk_t[:, blk:blk + 1], gain_k, cos_t, sin_t)
            kr[rows, :] = k_blk
            kx[:dim, rows] = jnp.transpose(k_blk)
            kx[dim:, rows] = ones
            vx[:dim, rows] = jnp.transpose(in_buf[slot, 3])
            vx[dim:, rows] = ones
    dkt[...] = jnp.zeros_like(dkt)
    dvt[...] = jnp.zeros_like(dvt)
    q_step, k_step = min(NQ_BLK, tok), NK_BLK
    per_blk = tok // q_step
    n_k = n_kb * tok

    for part in range(n_qp):
        base = part * n_part * tok

        def q_loop(qi, carry, part=part, base=base):
            qs = pl.ds(pl.multiple_of(base + qi * q_step, q_step), q_step)

            def one(j):
                ks = pl.ds(pl.multiple_of(j * k_step, k_step), k_step)
                s_mat = jnp.dot(qx[qs, :], kx[:, ks], preferred_element_type=F32)
                p_mat = jnp.exp2(s_mat * (scale * LOG2E))
                dp_mat = jnp.dot(dax[qs, :], vx[:, ks], preferred_element_type=F32)
                ds_low = (p_mat * dp_mat).astype(BF16)
                p_low = p_mat.astype(BF16)
                dvt[:, ks] += jnp.dot(dat[:, qs], p_low, preferred_element_type=F32)
                dkt[:, ks] += jnp.dot(qt[:, qs], ds_low, preferred_element_type=F32)
                return jnp.dot(ds_low, kr[ks, :], preferred_element_type=F32)

            def k_loop(jj, acc):
                for u in range(UNROLL):
                    acc = acc + one(jj * UNROLL + u)
                return acc

            acc = lax.fori_loop(0, n_k // k_step // UNROLL, k_loop, jnp.zeros((q_step, dim), F32))
            dq_refs[part][qi // per_blk, pl.ds(pl.multiple_of((qi % per_blk) * q_step, q_step), q_step), :] = acc
            return carry

        lax.fori_loop(0, n_part * per_blk, q_loop, 0)

    cs_copy(0).start()
    cs_copy(1).start()
    for blk in range(n_kb):
        rows = slice(blk * tok, (blk + 1) * tok)
        cos_t, sin_t = tables(blk, n_kb - 1)

        def unturned(total):
            low = (total * scale).astype(BF16).astype(F32)
            return low * cos_t - swap_pairs(low, lane) * sin_t

        if whole_q:
            dq_refs[0][blk] = unturned(dq_refs[0][blk])
        dk_ref[blk] = unturned(jnp.transpose(dkt[:, rows]))
        dv_ref[blk] = jnp.transpose(dvt[:, rows]).astype(BF16)


def attn_back(parts, n_kb, stats, gains, cs_all, scale):
    n_qp = len(parts)
    n_part, _, tok, dim = parts[0].shape
    n_q, n_k = n_qp * n_part * tok, n_kb * tok
    vm = pl.BlockSpec(memory_space=pltpu.VMEM)
    far = pl.BlockSpec(memory_space=pltpu.HBM)
    outs = tuple(jax.ShapeDtypeStruct((n_part, tok, dim), F32) for _ in range(n_qp))
    outs += (jax.ShapeDtypeStruct((n_kb, tok, dim), F32), jax.ShapeDtypeStruct((n_kb, tok, dim), BF16))
    return pl.pallas_call(
        functools.partial(attn_kernel, scale, n_q == n_k, n_qp),
        out_shape=outs,
        in_specs=[far] * n_qp + [vm] * 2 + [far],
        out_specs=(vm,) * (n_qp + 2),
        scratch_shapes=[
            pltpu.VMEM((n_q, 2 * dim), BF16), pltpu.VMEM((n_q, 2 * dim), BF16),
            pltpu.VMEM((2 * dim, n_k), BF16), pltpu.VMEM((2 * dim, n_k), BF16),
            pltpu.VMEM((dim, n_q), BF16), pltpu.VMEM((dim, n_q), BF16),
            pltpu.VMEM((n_k, dim), BF16),
            pltpu.VMEM((dim, n_k), F32), pltpu.VMEM((dim, n_k), F32),
            pltpu.VMEM((2, 4, tok, dim), BF16), pltpu.SemaphoreType.DMA((2,)),
            pltpu.VMEM((2, tok, dim), F32), pltpu.SemaphoreType.DMA((2,)),
        ],
        compiler_params=pltpu.CompilerParams(vmem_limit_bytes=VMEM_LIMIT),
        cost_estimate=pl.CostEstimate(flops=n_q * dim, bytes_accessed=n_q, transcendentals=0),
    )(*parts, stats, gains, cs_all)


def finish_kernel(scale, own_ref, got_ref, cs_ref, out_ref):
    tok, dim = own_ref.shape[1:]
    lane = lax.broadcasted_iota(jnp.int32, (tok, dim), 1)
    cos_t, sin_t = rope_tables(cs_ref[0], dim // 2)
    low = ((own_ref[0] + got_ref[0]) * scale).astype(BF16).astype(F32)
    out_ref[0] = low * cos_t - swap_pairs(low, lane) * sin_t


def finish_shared(own, got, cs_all, scale):
    blk = pl.BlockSpec((1,) + own.shape[1:], lambda i: (i, 0, 0))
    return pl.pallas_call(
        functools.partial(finish_kernel, scale), grid=(own.shape[0],),
        out_shape=jax.ShapeDtypeStruct(own.shape, F32),
        in_specs=[blk, blk, blk], out_specs=blk, name='finish_shared',
        cost_estimate=pl.CostEstimate(flops=own.size * 8, bytes_accessed=own.size * 16, transcendentals=0),
    )(own, got, cs_all)


def proj_kernel(n_solo, q_ref, k_ref, dr_ref, gate_ref, attn_ref, y_ref, wo_ref, wv_ref, bv_ref,
                do_ref, solo_ref, shared_ref, del_ref, dbo_ref):
    dim = solo_ref.shape[-1]
    rows, width = dr_ref.shape
    do = (dr_ref[...].astype(F32) * gate_ref[...]).astype(BF16)
    do_ref[...] = do

    @pl.when(pl.program_id(0) == 0)
    def _():
        dbo_ref[...] = jnp.zeros_like(dbo_ref)

    dbo_ref[...] += jnp.sum(do.astype(F32), axis=0, keepdims=True)
    lane = lax.broadcasted_iota(jnp.int32, (rows, dim), 1)
    d_attn = lax.dot_general(do, wo_ref[...], BY_TRANSPOSE, preferred_element_type=F32).astype(BF16)
    v_rows = (jnp.dot(y_ref[...], wv_ref[...], preferred_element_type=F32) + bv_ref[...]).astype(BF16)
    deltas = jnp.zeros((rows, dim), F32)
    for h in range(width // dim):
        cols = slice(h * dim, (h + 1) * dim)
        out = solo_ref.at[h] if h < n_solo else shared_ref.at[h - n_solo]
        out[0] = q_ref[:, cols]
        out[1] = d_attn[:, cols]
        out[2] = k_ref[:, cols]
        out[3] = v_rows[:, cols]
        row = jnp.sum(d_attn[:, cols].astype(F32) * attn_ref[:, cols].astype(F32), axis=1, keepdims=True)
        deltas = jnp.where(lane == h, row, deltas)
    del_ref[...] = jnp.transpose(deltas)[:del_ref.shape[0], :]


def project(pre_q, pre_k, d_resid, gate, attn, flat_y, w_o, w_v, b_v, n_solo, n_shared, dim):
    n_tok, width = d_resid.shape
    rows = 256
    tile = pl.BlockSpec((rows, width), lambda i: (i, 0))
    fixed = lambda shape: pl.BlockSpec(shape, lambda i: (0, 0))
    solo = pl.BlockSpec((n_solo, 4, rows, dim), lambda i: (0, 0, i, 0))
    shared = pl.BlockSpec((n_shared, 4, rows, dim), lambda i: (0, 0, i, 0))
    return pl.pallas_call(
        functools.partial(proj_kernel, n_solo), grid=(n_tok // rows,),
        out_shape=(jax.ShapeDtypeStruct((n_tok, width), BF16), jax.ShapeDtypeStruct((n_solo, 4, n_tok, dim), BF16),
                   jax.ShapeDtypeStruct((n_shared, 4, n_tok, dim), BF16),
                   jax.ShapeDtypeStruct((16, n_tok), F32), jax.ShapeDtypeStruct((1, width), F32)),
        in_specs=[tile, tile, tile, fixed((1, width)), tile, tile, fixed((width, width)), fixed((width, width)), fixed((1, width))],
        out_specs=(tile, solo, shared, pl.BlockSpec((16, rows), lambda i: (0, i)), fixed((1, width))),
        name='project', compiler_params=pltpu.CompilerParams(vmem_limit_bytes=VMEM_LIMIT),
        cost_estimate=pl.CostEstimate(flops=4 * n_tok * width * width, bytes_accessed=12 * n_tok * width * 2, transcendentals=0),
    )(pre_q, pre_k, d_resid, gate, attn, flat_y, w_o, w_v, b_v)


def grad_kernel(solo_ref, shared_ref, *refs):
    w_refs, out_ref = refs[:3], refs[3]
    total = None
    for i, w_ref in enumerate(w_refs):
        rows = jnp.concatenate([solo_ref[h, i] for h in range(solo_ref.shape[0])]
                               + [shared_ref[h, i] for h in range(shared_ref.shape[0])], axis=1)
        term = lax.dot_general(rows, w_ref[...], BY_TRANSPOSE, preferred_element_type=F32)
        total = term if total is None else total + term
    out_ref[...] = total.astype(BF16)


def grad_rows(solo_tok, shared_tok, weights):
    n_solo, _, n_tok, dim = solo_tok.shape
    n_shared = shared_tok.shape[0]
    width = weights[0].shape[0]
    rows = 256
    solo = pl.BlockSpec((n_solo, 3, rows, dim), lambda i: (0, 0, i, 0))
    shared = pl.BlockSpec((n_shared, 3, rows, dim), lambda i: (0, 0, i, 0))
    fixed = pl.BlockSpec((width, width), lambda i: (0, 0))
    return pl.pallas_call(
        grad_kernel, grid=(n_tok // rows,), out_shape=jax.ShapeDtypeStruct((n_tok, width), BF16),
        in_specs=[solo, shared] + [fixed] * 3, out_specs=pl.BlockSpec((rows, width), lambda i: (i, 0)),
        name='grad_rows', compiler_params=pltpu.CompilerParams(vmem_limit_bytes=VMEM_LIMIT),
        cost_estimate=pl.CostEstimate(flops=6 * n_tok * width * width, bytes_accessed=7 * n_tok * width * 2, transcendentals=0),
    )(solo_tok, shared_tok, *weights)


def assemble_kernel(first_ref, second_ref, out_ref):
    out_ref[...] = jnp.transpose(jnp.concatenate([first_ref[0], second_ref[0]], axis=0))


def assemble(full, which, n_solo, n_uly, n_heads, dim):
    width = full.shape[-1]
    half = dim // 2
    base = 3 * which

    def first(h):
        solo = h < n_solo
        return jnp.where(solo, h, h - n_solo), jnp.where(solo, base, base + 2), 0

    def second(h):
        solo = h < n_solo
        return jnp.where(solo, h, h - n_solo + n_uly), jnp.where(solo, base + 1, base + 2), 0

    return pl.pallas_call(
        assemble_kernel, grid=(n_heads,), out_shape=jax.ShapeDtypeStruct((width, width), F32),
        in_specs=[pl.BlockSpec((1, half, width), first), pl.BlockSpec((1, half, width), second)],
        out_specs=pl.BlockSpec((width, dim), lambda h: (0, h)), name='assemble',
        cost_estimate=pl.CostEstimate(flops=0, bytes_accessed=8 * width * width, transcendentals=0),
    )(full, full)


def solution(mesh):
    n_ring, n_uly = mesh.shape['ring'], mesh.shape['uly']
    n_grp = n_ring * n_uly
    ring_swap = [(idx, (idx + 1) % n_ring) for idx in range(n_ring)]
    tok_three = P('dp', GROUP, None)
    tok_two = P('dp', GROUP)
    whole = P()

    def device_fn(y_mod, pre_q, pre_k, inv_q, inv_k, log_sum, attn_out, gate, d_resid, angles, w_q, w_k, w_v, b_v, w_o, g_q, g_k):
        _, n_tok, width = y_mod.shape
        n_heads = log_sum.shape[1]
        dim = width // n_heads
        scale = dim ** -0.5
        n_solo, n_shared = n_grp, n_heads - n_grp
        ring_i, uly_i = lax.axis_index('ring'), lax.axis_index('uly')
        me = ring_i * n_uly + uly_i
        flat_y = y_mod.reshape(n_tok, width)

        def to_mine(arr, axes):
            return lax.all_to_all(arr, axes, 0, 0, tiled=True)

        def own_first(arr):
            flipped = jnp.concatenate([arr[n_uly:], arr[:n_uly]], axis=0)
            return jnp.where(ring_i == 0, arr, flipped)

        cs_own = jnp.concatenate([jnp.cos(angles), jnp.sin(angles)], axis=1)
        cs_all = lax.all_gather(cs_own, GROUP, axis=0)
        stat_own = jnp.concatenate([log_sum[0], inv_q, inv_k], axis=0)
        stat_all = lax.all_gather(stat_own, GROUP, axis=0)

        flat_attn = attn_out.reshape(n_tok, width)
        d_out, solo_s, shared_s, delta_own, db_o = project(
            pre_q.reshape(n_tok, width), pre_k.reshape(n_tok, width), d_resid.reshape(n_tok, width), gate, flat_attn, flat_y,
            w_o, w_v, b_v[None], n_solo, n_shared, dim)
        dw_o = lax.dot_general(flat_attn, d_out, (((0,), (0,)), ((), ())), preferred_element_type=F32)
        delta_all = lax.all_gather(delta_own, GROUP, axis=0)
        shared_s, dw_o, stat_all, delta_all = lax.optimization_barrier((shared_s, dw_o, stat_all, delta_all))
        dw_o = lax.psum(dw_o, ('dp', 'ring', 'uly'))
        shared_in = to_mine(shared_s, 'uly')
        shared_far = lax.ppermute(shared_in[:, :2], 'ring', ring_swap)

        def head_stats(head):
            return (lax.dynamic_index_in_dim(stat_all, head, 1, keepdims=False),
                    lax.dynamic_index_in_dim(delta_all, head, 1, keepdims=False))

        inv_q_all, inv_k_all = stat_all[:, n_heads], stat_all[:, n_heads + 1]
        lse_a, del_a = head_stats(me)
        lse_c, del_c = head_stats(n_solo + uly_i)
        stats_a = jnp.stack([lse_a, del_a, inv_q_all, inv_k_all])
        stats_c = jnp.stack([own_first(x) for x in (lse_c, del_c, inv_q_all, inv_k_all)])
        cs_c = own_first(cs_all)

        def head_gains(head):
            return jnp.concatenate([lax.dynamic_slice_in_dim(g, head * dim, dim, 0)[None] for g in (g_q, g_k)], axis=0)

        gains_a, gains_c = head_gains(me), head_gains(n_solo + uly_i)
        solo_s, shared_far, stats_c, stats_a, cs_c, gains_a, gains_c = lax.optimization_barrier(
            (solo_s, shared_far, stats_c, stats_a, cs_c, gains_a, gains_c))
        solo_in = to_mine(solo_s, GROUP)
        dqc_own, dqc_far, dnk_c, dvc = attn_back((shared_in, shared_far), n_uly, stats_c, gains_c, cs_c, scale)
        dqc_got = lax.ppermute(dqc_far, 'ring', ring_swap)
        dvc_got = lax.ppermute(dvc, 'ring', ring_swap)
        stats_a, late_y, dvc, solo_in = lax.optimization_barrier((stats_a, flat_y, dvc, solo_in))
        y_all = lax.all_gather(late_y, GROUP, axis=0)
        dnq_a, dnk_a, dva = attn_back((solo_in,), n_grp, stats_a, gains_a, cs_all, scale)
        dnq_a, dnk_a, dva, y_all, dqc_got, dvc_got, dw_o = lax.optimization_barrier((dnq_a, dnk_a, dva, y_all, dqc_got, dvc_got, dw_o))
        qa, ka, qc, kc = solo_in[:, 0], solo_in[:, 2], shared_in[:, 0], shared_in[:, 2]
        dnq_c = finish_shared(dqc_own, dqc_got, cs_c, scale)

        def partials(d_norm, proj, inv, gain):
            proj_f = proj.astype(F32)
            return jnp.sum(proj_f * gain * d_norm, axis=-1), jnp.sum(d_norm * proj_f * inv[..., None], axis=(0, 1))

        inv_c = (stats_c[2, :n_uly], stats_c[3, :n_uly])
        mq_a, dgq_a = partials(dnq_a, qa, inv_q_all, gains_a[0])
        mk_a, dgk_a = partials(dnk_a, ka, inv_k_all, gains_a[1])
        mq_c, dgq_c = partials(dnq_c, qc, inv_c[0], gains_c[0])
        mk_c, dgk_c = partials(dnk_c, kc, inv_c[1], gains_c[1])

        def place(own):
            zero = jnp.zeros_like(own)
            return jnp.where(ring_i == 0, jnp.concatenate([own, zero], 0), jnp.concatenate([zero, own], 0))

        mixed = jnp.sum(lax.all_gather(jnp.stack([mq_a + place(mq_c), mk_a + place(mk_c)]), GROUP, axis=0), axis=0) * (1.0 / width)
        mixed, dva_late = lax.optimization_barrier((mixed, dva))
        mixed_c = lax.dynamic_slice_in_dim(mixed, ring_i * n_uly, n_uly, 1)

        def back(d_norm, proj, inv, gain, mix):
            rms = inv[..., None]
            return (rms * gain * d_norm - proj.astype(F32) * rms ** 3 * mix[..., None]).astype(BF16)

        dpq_a = back(dnq_a, qa, inv_q_all, gains_a[0], mixed[0])
        dpk_a = back(dnk_a, ka, inv_k_all, gains_a[1], mixed[1])
        dpq_c = back(dnq_c, qc, inv_c[0], gains_c[0], mixed_c[0])
        dpk_c = back(dnk_c, kc, inv_c[1], gains_c[1], mixed_c[1])

        half = dim // 2

        def cut(arr):
            low, high = arr[..., :half], arr[..., half:]
            return jnp.where(ring_i == 0, low, high), jnp.where(ring_i == 0, high, low)

        (q_keep, q_send), (k_keep, k_send) = cut(dpq_c), cut(dpk_c)
        got = lax.ppermute(jnp.concatenate([q_send, k_send], axis=2), 'ring', ring_swap)

        def block(solo, keep, other):
            cols = jnp.where(ring_i == 0, jnp.concatenate([keep, other], 0), jnp.concatenate([other, keep], 0))
            rows = jnp.concatenate([solo, cols], axis=2)
            dw = lax.dot_general(rows, y_all, (((0, 1), (0, 1)), ((), ())), preferred_element_type=F32)
            return dw, jnp.sum(rows, axis=(0, 1), dtype=F32)

        blocks = [block(dva_late, cut(dvc)[0], cut(dvc_got)[0]), block(dpq_a, q_keep, got[..., :half]), block(dpk_a, k_keep, got[..., half:])]
        vecs = [b[1] for b in blocks] + [dgq_a, dgk_a, dgq_c, dgk_c]
        n_vec = sum(x.shape[0] for x in vecs)
        vec_row = jnp.concatenate(vecs + [jnp.zeros((width - n_vec,), F32)])[None]
        tail_rows = jnp.concatenate([vec_row, db_o, jnp.zeros((6, width), F32)], axis=0)
        n_row = dim + dim * n_shared // n_grp
        mine_v = lax.psum(blocks[0][0], 'dp')
        mine = lax.psum(jnp.concatenate([blocks[1][0], blocks[2][0], tail_rows], axis=0), 'dp')
        solo_ret, shared_ret, got = lax.optimization_barrier((jnp.stack([dpq_a, dpk_a, dva], axis=1), jnp.stack([dpq_c, dpk_c, dvc], axis=1), got))
        solo_tok, shared_tok = to_mine(solo_ret, GROUP), to_mine(shared_ret, 'uly')
        mine_all, solo_tok, shared_tok = lax.optimization_barrier((jnp.concatenate([mine_v, mine], axis=0), solo_tok, shared_tok))
        full = lax.all_gather(mine_all, GROUP, axis=0)

        def whole_dw(i):
            return assemble(full, i, n_solo, n_uly, n_heads, dim)

        def whole_db(i):
            part = full[:, 3 * n_row, i * n_row:(i + 1) * n_row]
            shared = part[:, dim:].reshape(n_ring, n_uly, n_row - dim).transpose(1, 0, 2).reshape(n_shared * dim)
            return jnp.concatenate([part[:, :dim].reshape(n_solo * dim), shared])

        def whole_dg(i):
            start = 3 * n_row
            solo = full[:, 3 * n_row, start + i * dim:start + (i + 1) * dim].reshape(n_solo * dim)
            shared = full[:, 3 * n_row, start + (2 + i) * dim:start + (3 + i) * dim].reshape(n_ring, n_uly, dim)
            return jnp.concatenate([solo, jnp.sum(shared, axis=0).reshape(n_shared * dim)])

        grad_y = grad_rows(solo_tok, shared_tok, (w_q, w_k, w_v)).reshape(y_mod.shape)
        db_o_all = jnp.sum(full[:, 3 * n_row + 1], axis=0)
        return (grad_y, whole_dw(1), whole_dw(2), whole_dw(0), dw_o, whole_db(1), whole_db(2), whole_db(0), db_o_all, whole_dg(0), whole_dg(1))

    in_specs = (tok_three, tok_three, tok_three, tok_two, tok_two, P('dp', None, GROUP), tok_three, P('dp', None), tok_three, P(GROUP, None), whole, whole, whole, whole, whole, whole, whole)
    out_specs = (tok_three, whole, whole, whole, whole, whole, whole, whole, whole, whole, whole)
    return jax.shard_map(device_fn, mesh=mesh, in_specs=in_specs, out_specs=out_specs, check_vma=False)
```
